32 devices in a mesh: box: 8 (over z, x), cone: 4 (over y, core).
Axes of the slice: x: 2, y: 2, z: 4, core: 2. Of those that a mesh axis runs over, the one named last changes fastest.
Arguments:
- leaf_factor: float32 [128, 96, 64, 64], P('box', 'cone'), may hold values from -0.6 to 0.6
- leaf_transfer: float32 [128, 96, 64, 64], P('box', 'cone'), may hold values from -0.5 to 0.5
- leaf_cone_map: int32 [96], P('cone'), may hold values from 0 to 95, as said below
- parent_transfer: float32 [16, 96, 64, 64], P('box', 'cone'), may hold values from -0.5 to 0.5
- parent_cone_map: int32 [96], P('cone'), may hold values from 0 to 95
- coupling: bfloat16 [16, 96, 8, 64, 64], P('box', 'cone'), may hold values from -6 to 6
- partner: int32 [16, 96, 8], P('box', 'cone'), may hold values from 0 to 15
- live: int32 [16, 96, 8], P('box', 'cone'), may hold values 0 or 1
Outputs:
- projected: bfloat16 [16, 96, 8, 64, 64], P('box', 'cone')
- new_transfer: float32 [16, 96, 64, 64], P('box', 'cone')
The draws below stay inside these ranges and needn't reach their ends.
Inputs may be any that keep to these rules, and one draw needn't show every extreme that they name: leaf_cone_map[c] lies within 24 positions of c, counted cyclically modulo 96.
All inputs are finite; a program needn't handle non-finite values. No bound on the sum of `live` on one device may be relied on, other than what follows from the above.
Results may differ from the reference program's by a relative error of at most 0.001.
Values sent between devices are 32-bit elements; how exact they have to be, the bound alone decides.
A program may use at most 192 MiB of HBM per device.

```python
import jax
import jax.numpy as jnp
from jax import lax

RANK = 64
CONES = 96
NBR = 8
CONE_DEV = 24
NB0 = 128
NB1 = 16


def draw_leaf_cone_map(key, part):
    offsets = jax.random.randint(jax.random.fold_in(key, 11), (CONES,), -CONE_DEV, CONE_DEV + 1, dtype=jnp.int32)
    return ((jnp.arange(CONES, dtype=jnp.int32) + offsets + CONES) % CONES).astype(jnp.int32)


def with_ends(drawn, stream_key, smallest, top_value):
    longest = drawn.shape.index(max(drawn.shape))
    spots = []
    for shift in (0, 1):
        where = [jax.random.randint(jax.random.fold_in(stream_key, axis), (), 0, length) for axis, length in enumerate(drawn.shape)]
        where[longest] = (where[longest] + shift) % drawn.shape[longest]
        spots.append(tuple(where))
    return drawn.at[spots[0]].set(smallest).at[spots[1]].set(top_value)


def shard_levels(stream_key, dims, split, low, high):
    factor_of = 1.0
    for axis_at, blocks in split:
        steps = jax.random.uniform(jax.random.fold_in(jax.random.fold_in(stream_key, 6), axis_at), (blocks,), jnp.float32, low / len(split), high / len(split))
        factor_of = factor_of * jnp.repeat(jnp.exp(steps), dims[axis_at] // blocks).reshape((-1,) + (1,) * (len(dims) - 1 - axis_at))
    return factor_of


def normal_values(rng, extent, deviation, bound, cuts=(), kind=jnp.bfloat16):
    entries = jax.random.normal(rng, extent, jnp.float32) * deviation
    if len(cuts) > 0:
        entries = shard_levels(rng, extent, cuts, -0.22, 0.18) * entries
    return jnp.clip(entries, min=-bound, max=bound).astype(kind)


def setup_inputs(seed: int = 0) -> dict:
    keys = jax.random.split(jax.random.key(seed), 9)
    return {
        "leaf_factor": normal_values(keys[0], (NB0, CONES, RANK, RANK), 0.1, 0.6, ((0, 8), (1, 4)), jnp.float32),
        "leaf_transfer": normal_values(keys[1], (NB0, CONES, RANK, RANK), 0.08, 0.5, ((0, 8), (1, 4)), jnp.float32),
        "leaf_cone_map": draw_leaf_cone_map(jax.random.fold_in(keys[8], 71), 0),
        "parent_transfer": normal_values(keys[3], (NB1, CONES, RANK, RANK), 0.08, 0.5, ((0, 8), (1, 4)), jnp.float32),
        "parent_cone_map": with_ends(jax.random.randint(keys[4], (CONES,), 0, CONES), jax.random.fold_in(keys[4], 1), 0, CONES - 1).astype(jnp.int32),
        "coupling": normal_values(keys[5], (NB1, CONES, NBR, RANK, RANK), 1.0, 6.0, ((0, 8), (1, 4))),
        "partner": with_ends(jax.random.randint(keys[6], (NB1, CONES, NBR), 0, NB1), jax.random.fold_in(keys[6], 1), 0, NB1 - 1).astype(jnp.int32),
        "live": with_ends((jax.random.randint(keys[7], (NB1, CONES, NBR), 0, 4) < 3).astype(jnp.int32), jax.random.fold_in(keys[7], 1), 0, 1),
    }


HIGHEST = lax.Precision.HIGHEST

def gram_factor(blocks, group_size):
    gram_sums = jnp.einsum('bcji,bcjk->bcik', blocks, blocks, precision=HIGHEST)
    count = gram_sums.shape[0] // group_size
    gram_sums = gram_sums.reshape((count, group_size) + gram_sums.shape[1:]).sum(1) / 8.0
    lower_part = jnp.linalg.cholesky(gram_sums)
    return jnp.swapaxes(lower_part, -1, -2)

def reference(leaf_factor, leaf_transfer, leaf_cone_map, parent_transfer, parent_cone_map, coupling, partner, live):
    identity = jnp.eye(RANK, dtype=jnp.float32)
    factor = leaf_factor + identity
    chosen = factor[:, leaf_cone_map]
    first_level = jnp.einsum('bcij,bcjk->bcik', chosen, leaf_transfer + identity, precision=HIGHEST)
    upper_one = gram_factor(first_level, 8)
    chosen_two = upper_one[:, parent_cone_map]
    second = jnp.einsum('bcij,bcjk->bcik', chosen_two, parent_transfer + identity, precision=HIGHEST)
    upper_two = jnp.repeat(gram_factor(second, 8), 8, axis=0)
    solved = jax.scipy.linalg.solve_triangular(jnp.swapaxes(upper_two, -1, -2), jnp.swapaxes(second, -1, -2), lower=True)
    new_transfer = jnp.swapaxes(solved, -1, -2)
    cone_ids = jnp.arange(CONES)

    def project(items):
        row_factor, blocks, mates, alive = items
        partner_side = upper_one[mates, cone_ids[:, None]]
        left_side = jnp.einsum('cij,cnjk->cnik', row_factor, blocks.astype(jnp.float32), precision=HIGHEST)
        whole_block = jnp.einsum('cnij,cnkj->cnik', left_side, partner_side, precision=HIGHEST)
        return (whole_block * alive[:, :, None, None].astype(jnp.float32)).astype(jnp.bfloat16)
    projected = lax.map(project, (upper_one, coupling, partner, live))
    return (projected, new_transfer)
```

```python
import functools

import jax
import jax.numpy as jnp
from jax import lax
from jax.experimental import pallas as pl
from jax.experimental.pallas import tpu as pltpu
from jax.sharding import PartitionSpec as P

HIGH = lax.Precision.HIGH
LEAVES = 8


def halves(value):
    top = value.astype(jnp.bfloat16)
    return top, (value - top.astype(jnp.float32)).astype(jnp.bfloat16)


def dot(a, b, dims):
    return lax.dot_general(a, b, (dims, ((), ())), preferred_element_type=jnp.float32)


def product(a, b, contract_b=0):
    a_top, a_low = halves(a)
    b_top, b_low = halves(b)
    dims = ((1,), (contract_b,))
    return dot(a_top, b_top, dims) + (dot(a_low, b_top, dims) + dot(a_top, b_low, dims))


def fold(block):
    half = block.shape[-2] // 2
    return jnp.concatenate([block[..., :half, :], block[..., half:, :]], axis=-1)


def unfold(block):
    half = block.shape[-1] // 2
    return jnp.concatenate([block[..., :half], block[..., half:]], axis=-2)


def gram_sum(rows):
    top, low = halves(rows)
    dims = ((0,), (0,))
    cross = dot(top, low, dims)
    return dot(top, top, dims) + (cross + cross.T)


def pack_kernel(picks_ref, factor_ref, out_ref):
    out_ref[...] = fold(factor_ref[...])


def pack(factor, picks):
    leaves, _, rank, _ = factor.shape
    count = picks.shape[0]
    return pl.pallas_call(
        pack_kernel,
        out_shape=jax.ShapeDtypeStruct((leaves, count, rank // 2, 2 * rank), factor.dtype),
        grid_spec=pltpu.PrefetchScalarGridSpec(
            num_scalar_prefetch=1,
            grid=(count,),
            in_specs=[pl.BlockSpec((leaves, 1, rank, rank), lambda k, picks: (0, picks[k], 0, 0))],
            out_specs=pl.BlockSpec((leaves, 1, rank // 2, 2 * rank), lambda k, picks: (0, k, 0, 0)),
        ),
        name="pack",
    )(picks, factor)


def identity_of(rank):
    rows = lax.broadcasted_iota(jnp.int32, (rank, rank), 0)
    columns = lax.broadcasted_iota(jnp.int32, (rank, rank), 1)
    return (rows == columns).astype(jnp.float32)


def leaf_kernel(side_ref, own_at, left_at, right_at, own_ref, left_ref, right_ref, move_ref, gram_ref, held, rows):
    c = pl.program_id(0)
    leaves, rank = held.shape[0], held.shape[-1]
    side = side_ref[c]

    @pl.when(side == 0)
    def _():
        held[...] = unfold(left_ref[:, 0])

    @pl.when(side == 1)
    def _():
        held[...] = own_ref[:, 0]

    @pl.when(side == 2)
    def _():
        held[...] = unfold(right_ref[:, 0])

    identity = identity_of(rank)
    for p in range(leaves // LEAVES):
        for leaf in range(LEAVES):
            at = p * LEAVES + leaf
            factor = held[at] + identity
            rows[p, pl.ds(leaf * rank, rank), :] = factor + product(factor, move_ref[at, 0])
        gram_ref[p, 0] = gram_sum(rows[p]) * (1.0 / LEAVES)


def leaf_grams(side, own_at, left_at, right_at, own, left, right, move):
    leaves, cones, rank, _ = own.shape
    parents = leaves // LEAVES
    whole = (leaves, 1, rank, rank)
    folded = (leaves, 1, rank // 2, 2 * rank)
    return pl.pallas_call(
        leaf_kernel,
        out_shape=jax.ShapeDtypeStruct((parents, cones, rank, rank), jnp.float32),
        grid_spec=pltpu.PrefetchScalarGridSpec(
            num_scalar_prefetch=4,
            grid=(cones,),
            in_specs=[
                pl.BlockSpec(whole, lambda c, s, o, l, r: (0, o[c], 0, 0)),
                pl.BlockSpec(folded, lambda c, s, o, l, r: (0, l[c], 0, 0)),
                pl.BlockSpec(folded, lambda c, s, o, l, r: (0, r[c], 0, 0)),
                pl.BlockSpec(whole, lambda c, s, o, l, r: (0, c, 0, 0)),
            ],
            out_specs=pl.BlockSpec((parents, 1, rank, rank), lambda c, s, o, l, r: (0, c, 0, 0)),
            scratch_shapes=[
                pltpu.VMEM((leaves, rank, rank), jnp.float32),
                pltpu.VMEM((parents, LEAVES * rank, rank), jnp.float32),
            ],
        ),
        name="leaf_grams",
    )(side, own_at, left_at, right_at, own, left, right, move)


def eliminate_kernel(inverse, gram_ref, upper_ref, *rest):
    if inverse:
        inverse_ref, work, solved = rest
    else:
        (work,) = rest
    rank, _, batch = gram_ref.shape
    work[...] = gram_ref[...]
    if inverse:
        shape = (rank, rank, batch)
        rows = lax.broadcasted_iota(jnp.int32, shape, 0)
        columns = lax.broadcasted_iota(jnp.int32, shape, 1)
        solved[...] = (rows == columns).astype(jnp.float32)
        inverse_ref[...] = jnp.zeros(shape, jnp.float32)
    tile = 8
    for block in range(rank // tile):
        low = block * tile
        width = rank - low
        if low:
            upper_ref[pl.ds(low, tile), pl.ds(0, low), :] = jnp.zeros((tile, low, batch), jnp.float32)

        def step(inner, carry, low=low, width=width):
            k = low + inner
            scale = 1.0 / jnp.sqrt(work[k, pl.ds(k, 1), :])
            places = low + lax.broadcasted_iota(jnp.int32, (width, batch), 0)
            row = jnp.where(places >= k, work[k, pl.ds(low, width), :] * scale, 0.0)
            upper_ref[k, pl.ds(low, width), :] = row
            if inverse:
                solved_row = solved[k, pl.ds(0, low + tile), :] * scale
                inverse_ref[k, pl.ds(0, low + tile), :] = solved_row
            for i in range(low, rank):
                weight = upper_ref[k, pl.ds(i, 1), :]
                start = (i // tile) * tile
                work[i, pl.ds(start, rank - start), :] = (
                    work[i, pl.ds(start, rank - start), :] - weight * row[start - low :]
                )
                if inverse:
                    solved[i, pl.ds(0, low + tile), :] = (
                        solved[i, pl.ds(0, low + tile), :] - weight * solved_row
                    )
            return carry

        lax.fori_loop(0, tile, step, 0)


def eliminate(grams, inverse):
    batch, rank, _ = grams.shape
    shape = jax.ShapeDtypeStruct((rank, rank, batch), jnp.float32)
    results = pl.pallas_call(
        functools.partial(eliminate_kernel, inverse),
        out_shape=[shape] * (1 + inverse),
        in_specs=[pl.BlockSpec(memory_space=pltpu.VMEM)],
        out_specs=[pl.BlockSpec(memory_space=pltpu.VMEM)] * (1 + inverse),
        scratch_shapes=[pltpu.VMEM(shape.shape, jnp.float32)] * (1 + inverse),
        name="eliminate",
    )(jnp.transpose(grams, (1, 2, 0)))
    return jnp.transpose(results[-1], (2, 0, 1))


def second_kernel(pick_ref, upper_ref, move_ref, second_ref, gram_ref, rows):
    parents, rank = move_ref.shape[0], move_ref.shape[-1]
    for p in range(parents):
        upper = unfold(upper_ref[0, p, 0])
        second = upper + product(upper, move_ref[p, 0])
        second_ref[p, 0] = second
        rows[pl.ds(p * rank, rank), :] = second
    gram_ref[0] = fold(gram_sum(rows[...]))


def second_level(picks, uppers, move):
    _, parents, cones, half, wide = uppers.shape
    rank = wide // 2
    whole = pl.BlockSpec((parents, 1, rank, rank), lambda c, picks: (0, c, 0, 0))
    return pl.pallas_call(
        second_kernel,
        out_shape=[
            jax.ShapeDtypeStruct(move.shape, jnp.float32),
            jax.ShapeDtypeStruct((cones, half, wide), jnp.float32),
        ],
        grid_spec=pltpu.PrefetchScalarGridSpec(
            num_scalar_prefetch=1,
            grid=(cones,),
            in_specs=[
                pl.BlockSpec(
                    (1, parents, 1, half, wide),
                    lambda c, picks: (picks[c] // cones, 0, picks[c] % cones, 0, 0),
                ),
                whole,
            ],
            out_specs=[whole, pl.BlockSpec((1, half, wide), lambda c, picks: (c, 0, 0))],
            scratch_shapes=[pltpu.VMEM((parents * rank, rank), jnp.float32)],
        ),
        name="second_level",
    )(picks, uppers, move)


def project_kernel(partner_ref, live_ref, own_ref, every_ref, coupling_ref, out_ref):
    c = pl.program_id(0)
    parents, slots = own_ref.shape[0], coupling_ref.shape[2]
    dims = ((1,), (0,))
    for t in range(parents):
        top, low = halves(unfold(own_ref[t, 0]))
        for j in range(slots):
            mate = unfold(every_ref[partner_ref[t, c, j], 0])
            block = coupling_ref[t, 0, j]
            left = dot(top, block, dims) + dot(low, block, dims)
            both = product(left, mate, 1)
            out_ref[t, 0, j] = (both * live_ref[t, c, j].astype(jnp.float32)).astype(out_ref.dtype)


def project(partner, live, own, every, coupling):
    parents, cones, slots, rank, _ = coupling.shape
    half, wide = own.shape[-2:]
    blocks = pl.BlockSpec((parents, 1, slots, rank, rank), lambda c, m, a: (0, c, 0, 0, 0))
    return pl.pallas_call(
        project_kernel,
        out_shape=jax.ShapeDtypeStruct(coupling.shape, coupling.dtype),
        grid_spec=pltpu.PrefetchScalarGridSpec(
            num_scalar_prefetch=2,
            grid=(cones,),
            in_specs=[
                pl.BlockSpec((parents, 1, half, wide), lambda c, m, a: (0, c, 0, 0)),
                pl.BlockSpec((every.shape[0], 1, half, wide), lambda c, m, a: (0, c, 0, 0)),
                blocks,
            ],
            out_specs=blocks,
        ),
        name="project",
    )(partner, live, own, every, coupling)


def partner_2(value, axis, bit):
    mask = 2**bit
    pairs = [(source, source ^ mask) for source in range(lax.axis_size(axis))]
    return lax.ppermute(value, axis, pairs)


def shards(
    leaf_factor,
    leaf_transfer,
    leaf_cone_map,
    parent_transfer,
    parent_cone_map,
    coupling,
    partner,
    live,
):
    leaves, cones, rank, _ = leaf_factor.shape
    parents = leaves // LEAVES
    count = lax.axis_size("cone")
    me = lax.axis_index("cone")

    maps = lax.all_gather(leaf_cone_map, "cone", axis=0, tiled=False)
    firsts = jnp.arange(count, dtype=jnp.int32)[:, None] * cones
    position = (maps - firsts + cones + count * cones) % (count * cones)
    side = position // cones
    place = position % cones
    is_side = (side[:, :, None] == jnp.arange(3)).astype(jnp.int32)
    order = jnp.cumsum(is_side, axis=1) - is_side
    slot = (order * is_side).sum(-1)
    busiest = jnp.maximum(is_side[..., 0].sum(1).max(), is_side[..., 2].sum(1).max())

    def listed(receiver, which, room):
        taken = (side[receiver] == which)[:, None] & (slot[receiver][:, None] == jnp.arange(room))
        return jnp.where(taken, place[receiver][:, None], 0).sum(0).astype(jnp.int32)

    def with_room(room):
        def run(factor, move):
            tail = pack(factor, listed((me + 1) % count, 0, room))
            head = pack(factor, listed((me + count - 1) % count, 2, room))
            left = lax.ppermute(tail, "cone", [(i, (i + 1) % count) for i in range(count)])
            right = lax.ppermute(head, "cone", [((i + 1) % count, i) for i in range(count)])
            mine, at = side[me], slot[me]
            return leaf_grams(
                mine,
                jnp.where(mine == 1, place[me], 0),
                jnp.where(mine == 0, at, 0),
                jnp.where(mine == 2, at, 0),
                factor,
                left,
                right,
                move,
            )

        return run

    room = (cones + 1) // 2
    gram_one = lax.cond(busiest <= room, with_room(room), with_room(cones), leaf_factor, leaf_transfer)

    upper_one = eliminate(gram_one.reshape((parents * cones, rank, rank)), False)
    upper_one = fold(upper_one).reshape((parents, cones, rank // 2, 2 * rank))
    segment = lax.all_gather(upper_one, "cone", axis=0, tiled=False)
    every_factor = lax.all_gather(upper_one, "box", axis=0, tiled=True)

    second, own_gram = second_level(parent_cone_map, segment, parent_transfer)
    group_size = LEAVES // parents
    summed = own_gram
    for bit_index in range(group_size.bit_length() - 1):
        summed = summed + partner_2(summed, "box", bit_index)
    inverse_two = eliminate(unfold(summed) / LEAVES, True)
    new_transfer = jnp.einsum("bcij,ckj->bcik", second, inverse_two, precision=HIGH)
    projected = project(partner, live, upper_one, every_factor, coupling)
    return (projected, new_transfer)


def solution(mesh):
    in_specs = (
        P("box", "cone", None, None),
        P("box", "cone", None, None),
        P("cone"),
        P("box", "cone", None, None),
        P("cone"),
        P("box", "cone", None, None, None),
        P("box", "cone", None),
        P("box", "cone", None),
    )
    out_specs = (P("box", "cone", None, None, None), P("box", "cone", None, None))
    return jax.shard_map(shards, mesh=mesh, in_specs=in_specs, out_specs=out_specs, check_vma=False)
```

```python
import functools

import jax
import jax.numpy as jnp
from jax import lax
from jax.experimental import pallas as pl
from jax.experimental.pallas import tpu as pltpu
from jax.sharding import PartitionSpec as P

HIGH = lax.Precision.HIGH
LEAVES = 8


def halves(value):
    top = value.astype(jnp.bfloat16)
    return top, (value - top.astype(jnp.float32)).astype(jnp.bfloat16)


def dot(a, b, dims):
    return lax.dot_general(a, b, (dims, ((), ())), preferred_element_type=jnp.float32)


def product(a, b, contract_b=0):
    a_top, a_low = halves(a)
    b_top, b_low = halves(b)
    dims = ((1,), (contract_b,))
    return dot(a_top, b_top, dims) + (dot(a_low, b_top, dims) + dot(a_top, b_low, dims))


def fold(block):
    half = block.shape[-2] // 2
    return jnp.concatenate([block[..., :half, :], block[..., half:, :]], axis=-1)


def unfold(block):
    half = block.shape[-1] // 2
    return jnp.concatenate([block[..., :half], block[..., half:]], axis=-2)


def gram_sum(rows):
    top, low = halves(rows)
    dims = ((0,), (0,))
    cross = dot(top, low, dims)
    return dot(top, top, dims) + (cross + cross.T)


def pack_kernel(picks_ref, factor_ref, out_ref):
    out_ref[...] = fold(factor_ref[...])


def pack(factor, picks):
    leaves, _, rank, _ = factor.shape
    count = picks.shape[0]
    return pl.pallas_call(
        pack_kernel,
        out_shape=jax.ShapeDtypeStruct((leaves, count, rank // 2, 2 * rank), factor.dtype),
        grid_spec=pltpu.PrefetchScalarGridSpec(
            num_scalar_prefetch=1,
            grid=(count,),
            in_specs=[pl.BlockSpec((leaves, 1, rank, rank), lambda k, picks: (0, picks[k], 0, 0))],
            out_specs=pl.BlockSpec((leaves, 1, rank // 2, 2 * rank), lambda k, picks: (0, k, 0, 0)),
        ),
        name="pack",
    )(picks, factor)


def identity_of(rank):
    rows = lax.broadcasted_iota(jnp.int32, (rank, rank), 0)
    columns = lax.broadcasted_iota(jnp.int32, (rank, rank), 1)
    return (rows == columns).astype(jnp.float32)


def leaf_products(held, move_ref, gram_ref, rows):
    leaves, rank = held.shape[0], held.shape[-1]
    identity = identity_of(rank)
    for p in range(leaves // LEAVES):
        for leaf in range(LEAVES):
            at = p * LEAVES + leaf
            factor = held[at] + identity
            rows[p, pl.ds(leaf * rank, rank), :] = factor + product(factor, move_ref[at, 0])
        gram_ref[p, 0] = gram_sum(rows[p]) * (1.0 / LEAVES)


def own_leaf_kernel(side_ref, own_at, own_ref, move_ref, gram_ref, rows):
    @pl.when(side_ref[pl.program_id(0)] == 1)
    def _():
        leaf_products(own_ref.at[:, 0], move_ref, gram_ref, rows)


def far_leaf_kernel(side_ref, left_at, right_at, left_ref, right_ref, move_ref, near_ref, gram_ref, held, rows):
    side = side_ref[pl.program_id(0)]

    @pl.when(side == 1)
    def _():
        gram_ref[...] = near_ref[...]

    @pl.when(side == 0)
    def _():
        held[...] = unfold(left_ref[:, 0])

    @pl.when(side == 2)
    def _():
        held[...] = unfold(right_ref[:, 0])

    @pl.when(side != 1)
    def _():
        leaf_products(held, move_ref, gram_ref, rows)


def leaf_cost(leaves, cones, rank):
    return pl.CostEstimate(
        flops=leaves * cones * rank**3 * 8, bytes_accessed=leaves * cones * rank**2 * 16, transcendentals=0
    )


def own_grams(side, own_at, own, move):
    leaves, cones, rank, _ = own.shape
    parents = leaves // LEAVES
    whole = (leaves, 1, rank, rank)
    return pl.pallas_call(
        own_leaf_kernel,
        out_shape=jax.ShapeDtypeStruct((parents, cones, rank, rank), jnp.float32),
        grid_spec=pltpu.PrefetchScalarGridSpec(
            num_scalar_prefetch=2,
            grid=(cones,),
            in_specs=[
                pl.BlockSpec(whole, lambda c, s, o: (0, o[c], 0, 0)),
                pl.BlockSpec(whole, lambda c, s, o: (0, c, 0, 0)),
            ],
            out_specs=pl.BlockSpec((parents, 1, rank, rank), lambda c, s, o: (0, c, 0, 0)),
            scratch_shapes=[pltpu.VMEM((parents, LEAVES * rank, rank), jnp.float32)],
        ),
        cost_estimate=leaf_cost(leaves, cones, rank),
        name="own_grams",
    )(side, own_at, own, move)


def far_grams(side, left_at, right_at, left, right, move, near):
    leaves, cones, rank, _ = move.shape
    parents = leaves // LEAVES
    whole = (leaves, 1, rank, rank)
    folded = (leaves, 1, rank // 2, 2 * rank)
    gram = pl.BlockSpec((parents, 1, rank, rank), lambda c, s, l, r: (0, c, 0, 0))
    return pl.pallas_call(
        far_leaf_kernel,
        out_shape=jax.ShapeDtypeStruct((parents, cones, rank, rank), jnp.float32),
        grid_spec=pltpu.PrefetchScalarGridSpec(
            num_scalar_prefetch=3,
            grid=(cones,),
            in_specs=[
                pl.BlockSpec(folded, lambda c, s, l, r: (0, l[c], 0, 0)),
                pl.BlockSpec(folded, lambda c, s, l, r: (0, r[c], 0, 0)),
                pl.BlockSpec(whole, lambda c, s, l, r: (0, c, 0, 0)),
                gram,
            ],
            out_specs=gram,
            scratch_shapes=[
                pltpu.VMEM((leaves, rank, rank), jnp.float32),
                pltpu.VMEM((parents, LEAVES * rank, rank), jnp.float32),
            ],
        ),
        cost_estimate=leaf_cost(leaves, cones, rank),
        name="far_grams",
    )(side, left_at, right_at, left, right, move, near)


def eliminate_kernel(inverse, gram_ref, upper_ref, *rest):
    if inverse:
        inverse_ref, work, solved = rest
    else:
        (work,) = rest
    rank, _, batch = gram_ref.shape
    work[...] = gram_ref[...]
    if inverse:
        shape = (rank, rank, batch)
        rows = lax.broadcasted_iota(jnp.int32, shape, 0)
        columns = lax.broadcasted_iota(jnp.int32, shape, 1)
        solved[...] = (rows == columns).astype(jnp.float32)
        inverse_ref[...] = jnp.zeros(shape, jnp.float32)
    tile = 8
    for block in range(rank // tile):
        low = block * tile
        width = rank - low
        if low:
            upper_ref[pl.ds(low, tile), pl.ds(0, low), :] = jnp.zeros((tile, low, batch), jnp.float32)

        def step(inner, carry, low=low, width=width):
            k = low + inner
            scale = 1.0 / jnp.sqrt(work[k, pl.ds(k, 1), :])
            places = low + lax.broadcasted_iota(jnp.int32, (width, batch), 0)
            row = jnp.where(places >= k, work[k, pl.ds(low, width), :] * scale, 0.0)
            upper_ref[k, pl.ds(low, width), :] = row
            if inverse:
                solved_row = solved[k, pl.ds(0, low + tile), :] * scale
                inverse_ref[k, pl.ds(0, low + tile), :] = solved_row
            for i in range(low, rank):
                weight = upper_ref[k, pl.ds(i, 1), :]
                start = (i // tile) * tile
                work[i, pl.ds(start, rank - start), :] = (
                    work[i, pl.ds(start, rank - start), :] - weight * row[start - low :]
                )
                if inverse:
                    solved[i, pl.ds(0, low + tile), :] = (
                        solved[i, pl.ds(0, low + tile), :] - weight * solved_row
                    )
            return carry

        lax.fori_loop(0, tile, step, 0)


def eliminate(grams, inverse):
    batch, rank, _ = grams.shape
    shape = jax.ShapeDtypeStruct((rank, rank, batch), jnp.float32)
    results = pl.pallas_call(
        functools.partial(eliminate_kernel, inverse),
        out_shape=[shape] * (1 + inverse),
        in_specs=[pl.BlockSpec(memory_space=pltpu.VMEM)],
        out_specs=[pl.BlockSpec(memory_space=pltpu.VMEM)] * (1 + inverse),
        scratch_shapes=[pltpu.VMEM(shape.shape, jnp.float32)] * (1 + inverse),
        name="eliminate",
    )(jnp.transpose(grams, (1, 2, 0)))
    return results[-1]


def pack_pair(columns):
    rank, cones = columns.shape[0], columns.shape[-1] // 2
    first = jnp.transpose(columns[..., :cones], (2, 0, 1))
    second = jnp.transpose(columns[..., cones:], (2, 1, 0))
    above = jnp.arange(rank)[:, None] <= jnp.arange(rank)[None, :]
    on = jnp.arange(rank)[:, None] == jnp.arange(rank)[None, :]
    diagonal = jnp.where(on, second, 0.0).sum(1)
    blocks = fold(jnp.where(above, first, second))
    last = jnp.pad(diagonal, ((0, rank // 2 - cones), (0, rank)))
    return jnp.concatenate([blocks, last[None]], axis=0)


def unpack_pair(block, diagonal):
    whole = unfold(block)
    rank = whole.shape[-1]
    rows = lax.broadcasted_iota(jnp.int32, (rank, rank), 0)
    columns = lax.broadcasted_iota(jnp.int32, (rank, rank), 1)
    first = jnp.where(rows <= columns, whole, 0.0)
    second = jnp.where(rows > columns, whole, jnp.where(rows == columns, diagonal[:, :rank], 0.0))
    return first, second


def second_kernel(pick_ref, pair_ref, last_ref, move_ref, second_ref, gram_ref, rows):
    parents, rank = move_ref.shape[0], move_ref.shape[-1]
    cones = pl.num_programs(0)
    at = pick_ref[pl.program_id(0)] % cones
    first, other = unpack_pair(pair_ref[0, 0], last_ref[0, 0, pl.ds(at, 1), :])
    for p, upper in enumerate((first, other.T)):
        second = upper + product(upper, move_ref[p, 0])
        second_ref[p, 0] = second
        rows[pl.ds(p * rank, rank), :] = second
    gram_ref[0] = fold(gram_sum(rows[...]))


def second_level(picks, pairs, move):
    parents, cones, rank, _ = move.shape
    half, wide = pairs.shape[-2:]
    whole = pl.BlockSpec((parents, 1, rank, rank), lambda c, picks: (0, c, 0, 0))
    return pl.pallas_call(
        second_kernel,
        out_shape=[
            jax.ShapeDtypeStruct(move.shape, jnp.float32),
            jax.ShapeDtypeStruct((cones, half, wide), jnp.float32),
        ],
        grid_spec=pltpu.PrefetchScalarGridSpec(
            num_scalar_prefetch=1,
            grid=(cones,),
            in_specs=[
                pl.BlockSpec((1, 1, half, wide), lambda c, picks: (picks[c] // cones, picks[c] % cones, 0, 0)),
                pl.BlockSpec((1, 1, half, wide), lambda c, picks: (picks[c] // cones, cones, 0, 0)),
                whole,
            ],
            out_specs=[whole, pl.BlockSpec((1, half, wide), lambda c, picks: (c, 0, 0))],
            scratch_shapes=[pltpu.VMEM((parents * rank, rank), jnp.float32)],
        ),
        cost_estimate=pl.CostEstimate(
            flops=parents * cones * rank**3 * 8, bytes_accessed=parents * cones * rank**2 * 16, transcendentals=0
        ),
        name="second_level",
    )(picks, pairs, pairs, move)


def project_kernel(partner_ref, live_ref, own_ref, every_ref, last_ref, coupling_ref, out_ref, tops, lows):
    c = pl.program_id(0)
    parents, rank, slots = own_ref.shape[0], own_ref.shape[-1], coupling_ref.shape[2]
    for d in range(every_ref.shape[0]):
        first, other = unpack_pair(every_ref[d, 0], last_ref[d, 0, pl.ds(c, 1), :])
        tops[2 * d], lows[2 * d] = halves(first.T)
        tops[2 * d + 1], lows[2 * d + 1] = halves(other)
    dims = ((1,), (0,))
    for t in range(parents):
        stack = jnp.concatenate(halves(own_ref[t, 0]), axis=0)
        for j in range(slots):
            mate = partner_ref[t, c, j]
            left = dot(stack, coupling_ref[t, 0, j], dims)
            top, low = halves(left[:rank] + left[rank:])
            both = dot(jnp.concatenate([top, low], axis=0), tops[mate], dims)
            both = both[:rank] + (both[rank:] + dot(top, lows[mate], dims))
            out_ref[t, 0, j] = (both * live_ref[t, c, j].astype(jnp.float32)).astype(out_ref.dtype)


def project(partner, live, own, every, coupling):
    parents, cones, slots, rank, _ = coupling.shape
    others, _, half, wide = every.shape
    blocks = pl.BlockSpec((parents, 1, slots, rank, rank), lambda c, m, a: (0, c, 0, 0, 0))
    return pl.pallas_call(
        project_kernel,
        out_shape=jax.ShapeDtypeStruct(coupling.shape, coupling.dtype),
        grid_spec=pltpu.PrefetchScalarGridSpec(
            num_scalar_prefetch=2,
            grid=(cones,),
            in_specs=[
                pl.BlockSpec((parents, 1, rank, rank), lambda c, m, a: (0, c, 0, 0)),
                pl.BlockSpec((others, 1, half, wide), lambda c, m, a: (0, c, 0, 0)),
                pl.BlockSpec((others, 1, half, wide), lambda c, m, a: (0, cones, 0, 0)),
                blocks,
            ],
            out_specs=blocks,
            scratch_shapes=[pltpu.VMEM((parents * others, rank, rank), jnp.bfloat16)] * 2,
        ),
        cost_estimate=pl.CostEstimate(
            flops=parents * cones * slots * rank**3 * 10,
            bytes_accessed=parents * cones * slots * rank**2 * 8,
            transcendentals=0,
        ),
        name="project",
    )(partner, live, own, every, every, coupling)


def partner_2(value, axis, bit):
    mask = 2**bit
    pairs = [(source, source ^ mask) for source in range(lax.axis_size(axis))]
    return lax.ppermute(value, axis, pairs)


def shards(
    leaf_factor,
    leaf_transfer,
    leaf_cone_map,
    parent_transfer,
    parent_cone_map,
    coupling,
    partner,
    live,
):
    leaves, cones, rank, _ = leaf_factor.shape
    parents = leaves // LEAVES
    count = lax.axis_size("cone")
    me = lax.axis_index("cone")

    maps = lax.all_gather(leaf_cone_map, "cone", axis=0, tiled=False)
    firsts = jnp.arange(count, dtype=jnp.int32)[:, None] * cones
    position = (maps - firsts + cones + count * cones) % (count * cones)
    every_place = jnp.arange(3 * cones, dtype=jnp.int32)
    used = (position[:, :, None] == every_place).any(1).reshape((count, 3, cones))
    used = used.astype(jnp.int32)
    earlier = jnp.arange(cones)[:, None] < jnp.arange(cones)[None, :]
    rank_of = (used[..., :, None] * earlier.astype(jnp.int32)).sum(2)
    totals = used.sum(2)
    busiest = jnp.maximum(totals[:, 0].max(), totals[:, 2].max())

    def listed(receiver, which, room):
        here = (rank_of[receiver, which][:, None] == jnp.arange(room)) & (used[receiver, which] > 0)[:, None]
        return jnp.where(here, jnp.arange(cones, dtype=jnp.int32)[:, None], 0).sum(0).astype(jnp.int32)

    mine = position[me]
    side, place = mine // cones, mine % cones
    slots = (jnp.where(mine[:, None] == every_place, rank_of[me].reshape(-1), 0)).sum(1).astype(jnp.int32)

    def with_room(room):
        def run(factor, move):
            tail = pack(factor, listed((me + 1) % count, 0, room))
            left = lax.ppermute(tail, "cone", [(i, (i + 1) % count) for i in range(count)])
            head = pack(factor, listed((me + count - 1) % count, 2, room))
            right = lax.ppermute(head, "cone", [((i + 1) % count, i) for i in range(count)])
            near = own_grams(side, jnp.where(side == 1, place, 0), factor, move)
            left_at, right_at = jnp.where(side == 0, slots, 0), jnp.where(side == 2, slots, 0)
            return far_grams(side, left_at, right_at, left, right, move, near)

        return run

    rooms = [max(1, cones * eighth // 24) for eighth in (7, 8, 9, 10, 12)] + [cones]
    branch = (busiest > jnp.array(rooms[:-1], jnp.int32)).astype(jnp.int32).sum()
    gram_one = lax.switch(branch, [with_room(room) for room in rooms], leaf_factor, leaf_transfer)

    columns = eliminate(gram_one.reshape((parents * cones, rank, rank)), False)
    pairs = pack_pair(columns)
    segment = lax.all_gather(pairs, "cone", axis=0, tiled=False)
    every_factor = lax.all_gather(pairs, "box", axis=0, tiled=False)
    upper_one = jnp.transpose(columns, (2, 0, 1)).reshape((parents, cones, rank, rank))

    second, own_gram = second_level(parent_cone_map, segment, parent_transfer)
    group_size = LEAVES // parents
    summed = own_gram
    for bit_index in range(group_size.bit_length() - 1):
        summed = summed + partner_2(summed, "box", bit_index)
    inverse_two = jnp.transpose(eliminate(unfold(summed) / LEAVES, True), (2, 0, 1))
    new_transfer = jnp.einsum("bcij,ckj->bcik", second, inverse_two, precision=HIGH)
    projected = project(partner, live, upper_one, every_factor, coupling)
    return (projected, new_transfer)


def solution(mesh):
    in_specs = (
        P("box", "cone", None, None),
        P("box", "cone", None, None),
        P("cone"),
        P("box", "cone", None, None),
        P("cone"),
        P("box", "cone", None, None, None),
        P("box", "cone", None),
        P("box", "cone", None),
    )
    out_specs = (P("box", "cone", None, None, None), P("box", "cone", None, None))
    return jax.shard_map(shards, mesh=mesh, in_specs=in_specs, out_specs=out_specs, check_vma=False)
```

```python
import functools

import jax
import jax.numpy as jnp
from jax import lax
from jax.experimental import pallas as pl
from jax.experimental.pallas import tpu as pltpu
from jax.sharding import PartitionSpec as P

HIGH = lax.Precision.HIGH
LEAVES = 8


def halves(value):
    top = value.astype(jnp.bfloat16)
    return top, (value - top.astype(jnp.float32)).astype(jnp.bfloat16)


def dot(a, b, dims):
    return lax.dot_general(a, b, (dims, ((), ())), preferred_element_type=jnp.float32)


def product(a, b, contract_b=0):
    a_top, a_low = halves(a)
    b_top, b_low = halves(b)
    dims = ((1,), (contract_b,))
    return dot(a_top, b_top, dims) + (dot(a_low, b_top, dims) + dot(a_top, b_low, dims))


def paired_product(a, b):
    size = a.shape[0]
    rows = jnp.concatenate(halves(a), axis=0)
    columns = jnp.concatenate(halves(b), axis=1)
    every = dot(rows, columns, ((1,), (0,)))
    return every[:size, :size] + (every[size:, :size] + every[:size, size:])


def fold(block):
    half = block.shape[-2] // 2
    return jnp.concatenate([block[..., :half, :], block[..., half:, :]], axis=-1)


def unfold(block):
    half = block.shape[-1] // 2
    return jnp.concatenate([block[..., :half], block[..., half:]], axis=-2)


def gram_sum(rows):
    top, low = halves(rows)
    dims = ((0,), (0,))
    cross = dot(top, low, dims)
    return dot(top, top, dims) + (cross + cross.T)


def pack_kernel(picks_ref, *refs):
    for g, factor_ref in enumerate(refs[:-1]):
        refs[-1][:, g] = fold(factor_ref[:, 0])


def pack(factor, picks):
    leaves, _, rank, _ = factor.shape
    count = picks.shape[0]
    group = group_of(count, 2)
    folded = (leaves, group, rank // 2, 2 * rank)
    return pl.pallas_call(
        pack_kernel,
        out_shape=jax.ShapeDtypeStruct((leaves, count, rank // 2, 2 * rank), factor.dtype),
        grid_spec=pltpu.PrefetchScalarGridSpec(
            num_scalar_prefetch=1,
            grid=(count // group,),
            in_specs=[
                pl.BlockSpec((leaves, 1, rank, rank), lambda k, picks, g=g: (0, picks[k * group + g], 0, 0))
                for g in range(group)
            ],
            out_specs=pl.BlockSpec(folded, lambda k, picks: (0, k, 0, 0)),
        ),
        name="pack",
    )(picks, *([factor] * group))


def identity_of(rank):
    rows = lax.broadcasted_iota(jnp.int32, (rank, rank), 0)
    columns = lax.broadcasted_iota(jnp.int32, (rank, rank), 1)
    return (rows == columns).astype(jnp.float32)


def group_of(cones, limit):
    return max(size for size in range(1, limit + 1) if cones % size == 0)


def leaf_products(held, move_ref, gram_ref, rows, g):
    leaves, rank = held.shape[0], held.shape[-1]
    identity = identity_of(rank)
    for p in range(leaves // LEAVES):
        for leaf in range(LEAVES):
            at = p * LEAVES + leaf
            factor = held[at] + identity
            rows[p, pl.ds(leaf * rank, rank), :] = factor + paired_product(factor, move_ref[at, g])
        gram_ref[p, g] = gram_sum(rows[p]) * (1.0 / LEAVES)


def own_leaf_kernel(group, side_ref, own_at, *refs):
    move_ref, gram_ref, rows = refs[group:]
    for g in range(group):

        @pl.when(side_ref[pl.program_id(0) * group + g] == 1)
        def _(g=g):
            leaf_products(refs[g].at[:, 0], move_ref, gram_ref, rows, g)


def far_leaf_kernel(group, side_ref, left_at, right_at, *refs):
    move_ref, near_ref, gram_ref, held, rows = refs[2 * group :]
    for g in range(group):
        side = side_ref[pl.program_id(0) * group + g]

        @pl.when(side == 1)
        def _(g=g):
            gram_ref[:, g] = near_ref[:, g]

        @pl.when(side == 0)
        def _(g=g):
            held[...] = unfold(refs[g][:, 0])

        @pl.when(side == 2)
        def _(g=g):
            held[...] = unfold(refs[group + g][:, 0])

        @pl.when(side != 1)
        def _(g=g):
            leaf_products(held, move_ref, gram_ref, rows, g)


def leaf_cost(leaves, cones, rank):
    return pl.CostEstimate(
        flops=leaves * cones * rank**3 * 8, bytes_accessed=leaves * cones * rank**2 * 16, transcendentals=0
    )


def own_grams(side, own_at, own, move):
    leaves, cones, rank, _ = own.shape
    parents = leaves // LEAVES
    group = group_of(cones, 2)
    return pl.pallas_call(
        functools.partial(own_leaf_kernel, group),
        out_shape=jax.ShapeDtypeStruct((parents, cones, rank, rank), jnp.float32),
        grid_spec=pltpu.PrefetchScalarGridSpec(
            num_scalar_prefetch=2,
            grid=(cones // group,),
            in_specs=[
                pl.BlockSpec((leaves, 1, rank, rank), lambda c, s, o, g=g: (0, o[c * group + g], 0, 0))
                for g in range(group)
            ]
            + [pl.BlockSpec((leaves, group, rank, rank), lambda c, s, o: (0, c, 0, 0))],
            out_specs=pl.BlockSpec((parents, group, rank, rank), lambda c, s, o: (0, c, 0, 0)),
            scratch_shapes=[pltpu.VMEM((parents, LEAVES * rank, rank), jnp.float32)],
        ),
        cost_estimate=leaf_cost(leaves, cones, rank),
        name="own_grams",
    )(side, own_at, *([own] * group), move)


def far_grams(side, left_at, right_at, left, right, move, near):
    leaves, cones, rank, _ = move.shape
    parents = leaves // LEAVES
    group = group_of(cones, 2)
    folded = (leaves, 1, rank // 2, 2 * rank)
    gram = pl.BlockSpec((parents, group, rank, rank), lambda c, s, l, r: (0, c, 0, 0))
    return pl.pallas_call(
        functools.partial(far_leaf_kernel, group),
        out_shape=jax.ShapeDtypeStruct((parents, cones, rank, rank), jnp.float32),
        grid_spec=pltpu.PrefetchScalarGridSpec(
            num_scalar_prefetch=3,
            grid=(cones // group,),
            in_specs=[pl.BlockSpec(folded, lambda c, s, l, r, g=g: (0, l[c * group + g], 0, 0)) for g in range(group)]
            + [pl.BlockSpec(folded, lambda c, s, l, r, g=g: (0, r[c * group + g], 0, 0)) for g in range(group)]
            + [pl.BlockSpec((leaves, group, rank, rank), lambda c, s, l, r: (0, c, 0, 0)), gram],
            out_specs=gram,
            scratch_shapes=[
                pltpu.VMEM((leaves, rank, rank), jnp.float32),
                pltpu.VMEM((parents, LEAVES * rank, rank), jnp.float32),
            ],
        ),
        cost_estimate=leaf_cost(leaves, cones, rank),
        name="far_grams",
    )(side, left_at, right_at, *([left] * group), *([right] * group), move, near)


def eliminate_kernel(inverse, gram_ref, upper_ref, *rest):
    if inverse:
        inverse_ref, work, solved = rest
    else:
        (work,) = rest
    rank, _, batch = gram_ref.shape
    work[...] = gram_ref[...]
    if inverse:
        shape = (rank, rank, batch)
        rows = lax.broadcasted_iota(jnp.int32, shape, 0)
        columns = lax.broadcasted_iota(jnp.int32, shape, 1)
        solved[...] = (rows == columns).astype(jnp.float32)
        inverse_ref[...] = jnp.zeros(shape, jnp.float32)
    tile = 8
    for block in range(rank // tile):
        low = block * tile
        width = rank - low
        if low:
            upper_ref[pl.ds(low, tile), pl.ds(0, low), :] = jnp.zeros((tile, low, batch), jnp.float32)

        def step(inner, carry, low=low, width=width):
            k = low + inner
            scale = 1.0 / jnp.sqrt(work[k, pl.ds(k, 1), :])
            places = low + lax.broadcasted_iota(jnp.int32, (width, batch), 0)
            row = jnp.where(places >= k, work[k, pl.ds(low, width), :] * scale, 0.0)
            upper_ref[k, pl.ds(low, width), :] = row
            if inverse:
                solved_row = solved[k, pl.ds(0, low + tile), :] * scale
                inverse_ref[k, pl.ds(0, low + tile), :] = solved_row
            for i in range(low, rank):
                weight = upper_ref[k, pl.ds(i, 1), :]
                start = (i // tile) * tile
                work[i, pl.ds(start, rank - start), :] = (
                    work[i, pl.ds(start, rank - start), :] - weight * row[start - low :]
                )
                if inverse:
                    solved[i, pl.ds(0, low + tile), :] = (
                        solved[i, pl.ds(0, low + tile), :] - weight * solved_row
                    )
            return carry

        lax.fori_loop(0, tile, step, 0)


def eliminate(grams, inverse):
    batch, rank, _ = grams.shape
    shape = jax.ShapeDtypeStruct((rank, rank, batch), jnp.float32)
    results = pl.pallas_call(
        functools.partial(eliminate_kernel, inverse),
        out_shape=[shape] * (1 + inverse),
        in_specs=[pl.BlockSpec(memory_space=pltpu.VMEM)],
        out_specs=[pl.BlockSpec(memory_space=pltpu.VMEM)] * (1 + inverse),
        scratch_shapes=[pltpu.VMEM(shape.shape, jnp.float32)] * (1 + inverse),
        name="eliminate",
    )(jnp.transpose(grams, (1, 2, 0)))
    return results[-1]


def pack_pair(columns):
    rank, cones = columns.shape[0], columns.shape[-1] // 2
    first = jnp.transpose(columns[..., :cones], (2, 0, 1))
    second = jnp.transpose(columns[..., cones:], (2, 1, 0))
    above = jnp.arange(rank)[:, None] <= jnp.arange(rank)[None, :]
    on = jnp.arange(rank)[:, None] == jnp.arange(rank)[None, :]
    diagonal = jnp.where(on, second, 0.0).sum(1)
    blocks = fold(jnp.where(above, first, second))
    last = jnp.pad(diagonal, ((0, rank // 2 - cones), (0, rank)))
    return jnp.concatenate([blocks, last[None]], axis=0)


def unpack_pair(block, diagonal):
    whole = unfold(block)
    rank = whole.shape[-1]
    rows = lax.broadcasted_iota(jnp.int32, (rank, rank), 0)
    columns = lax.broadcasted_iota(jnp.int32, (rank, rank), 1)
    first = jnp.where(rows <= columns, whole, 0.0)
    second = jnp.where(rows > columns, whole, jnp.where(rows == columns, diagonal[:, :rank], 0.0))
    return first, second


def second_kernel(group, pick_ref, pair_ref, move_ref, second_ref, gram_ref, rows):
    parents, rank = move_ref.shape[0], move_ref.shape[-1]
    cones = pl.num_programs(0) * group
    for g in range(group):
        pick = pick_ref[pl.program_id(0) * group + g]
        owner, at = pick // cones, pick % cones
        first, other = unpack_pair(pair_ref[owner, at], pair_ref[owner, cones, pl.ds(at, 1), :])
        for p, upper in enumerate((first, other.T)):
            second = upper + product(upper, move_ref[p, g])
            second_ref[p, g] = second
            rows[g, pl.ds(p * rank, rank), :] = second
        gram_ref[g] = fold(gram_sum(rows[g]))


def second_level(picks, pairs, move):
    parents, cones, rank, _ = move.shape
    half, wide = pairs.shape[-2:]
    group = group_of(cones, 4)
    whole = pl.BlockSpec((parents, group, rank, rank), lambda c, picks: (0, c, 0, 0))
    return pl.pallas_call(
        functools.partial(second_kernel, group),
        out_shape=[
            jax.ShapeDtypeStruct(move.shape, jnp.float32),
            jax.ShapeDtypeStruct((cones, half, wide), jnp.float32),
        ],
        grid_spec=pltpu.PrefetchScalarGridSpec(
            num_scalar_prefetch=1,
            grid=(cones // group,),
            in_specs=[pl.BlockSpec(pairs.shape, lambda c, picks: (0, 0, 0, 0)), whole],
            out_specs=[whole, pl.BlockSpec((group, half, wide), lambda c, picks: (c, 0, 0))],
            scratch_shapes=[pltpu.VMEM((group, parents * rank, rank), jnp.float32)],
        ),
        cost_estimate=pl.CostEstimate(
            flops=parents * cones * rank**3 * 8, bytes_accessed=parents * cones * rank**2 * 16, transcendentals=0
        ),
        name="second_level",
    )(picks, pairs, move)


def project_kernel(partner_ref, live_ref, own_ref, every_ref, last_ref, coupling_ref, out_ref, tops, lows):
    parents, group, rank, slots = own_ref.shape[0], own_ref.shape[1], own_ref.shape[-1], coupling_ref.shape[2]
    dims = ((1,), (0,))

    def step(g, carry):
        c = pl.program_id(0) * group + g
        for d in range(every_ref.shape[0]):
            first, other = unpack_pair(every_ref[d, g], last_ref[d, 0, pl.ds(c, 1), :])
            tops[2 * d], lows[2 * d] = halves(first.T)
            tops[2 * d + 1], lows[2 * d + 1] = halves(other)
        for t in range(parents):
            stack = jnp.concatenate(halves(own_ref[t, g]), axis=0)
            for j in range(slots):
                mate = partner_ref[t, c, j]
                left = dot(stack, coupling_ref[t, g, j], dims)
                top, low = halves(left[:rank] + left[rank:])
                both = dot(jnp.concatenate([top, low], axis=0), tops[mate], dims)
                both = both[:rank] + (both[rank:] + dot(top, lows[mate], dims))
                out_ref[t, g, j] = (both * live_ref[t, c, j].astype(jnp.float32)).astype(out_ref.dtype)
        return carry

    lax.fori_loop(0, group, step, 0)


def project(partner, live, own, every, coupling):
    parents, cones, slots, rank, _ = coupling.shape
    others, _, half, wide = every.shape
    group = group_of(cones, 4)
    blocks = pl.BlockSpec((parents, group, slots, rank, rank), lambda c, m, a: (0, c, 0, 0, 0))
    return pl.pallas_call(
        project_kernel,
        out_shape=jax.ShapeDtypeStruct(coupling.shape, coupling.dtype),
        grid_spec=pltpu.PrefetchScalarGridSpec(
            num_scalar_prefetch=2,
            grid=(cones // group,),
            in_specs=[
                pl.BlockSpec((parents, group, rank, rank), lambda c, m, a: (0, c, 0, 0)),
                pl.BlockSpec((others, group, half, wide), lambda c, m, a: (0, c, 0, 0)),
                pl.BlockSpec((others, 1, half, wide), lambda c, m, a: (0, cones, 0, 0)),
                blocks,
            ],
            out_specs=blocks,
            scratch_shapes=[pltpu.VMEM((parents * others, rank, rank), jnp.bfloat16)] * 2,
        ),
        cost_estimate=pl.CostEstimate(
            flops=parents * cones * slots * rank**3 * 10,
            bytes_accessed=parents * cones * slots * rank**2 * 8,
            transcendentals=0,
        ),
        name="project",
    )(partner, live, own, every, every, coupling)


def partner_2(value, axis, bit):
    mask = 2**bit
    pairs = [(source, source ^ mask) for source in range(lax.axis_size(axis))]
    return lax.ppermute(value, axis, pairs)


def shards(
    leaf_factor,
    leaf_transfer,
    leaf_cone_map,
    parent_transfer,
    parent_cone_map,
    coupling,
    partner,
    live,
):
    leaves, cones, rank, _ = leaf_factor.shape
    parents = leaves // LEAVES
    count = lax.axis_size("cone")
    me = lax.axis_index("cone")

    maps = lax.all_gather(leaf_cone_map, "cone", axis=0, tiled=False)
    firsts = jnp.arange(count, dtype=jnp.int32)[:, None] * cones
    position = (maps - firsts + cones + count * cones) % (count * cones)
    every_place = jnp.arange(3 * cones, dtype=jnp.int32)
    used = (position[:, :, None] == every_place).any(1).reshape((count, 3, cones))
    used = used.astype(jnp.int32)
    earlier = jnp.arange(cones)[:, None] < jnp.arange(cones)[None, :]
    rank_of = (used[..., :, None] * earlier.astype(jnp.int32)).sum(2)
    totals = used.sum(2)
    busiest = jnp.maximum(totals[:, 0].max(), totals[:, 2].max())

    def listed(receiver, which, room):
        here = (rank_of[receiver, which][:, None] == jnp.arange(room)) & (used[receiver, which] > 0)[:, None]
        return jnp.where(here, jnp.arange(cones, dtype=jnp.int32)[:, None], 0).sum(0).astype(jnp.int32)

    mine = position[me]
    side, place = mine // cones, mine % cones
    slots = (jnp.where(mine[:, None] == every_place, rank_of[me].reshape(-1), 0)).sum(1).astype(jnp.int32)

    def with_room(room):
        def run(factor, move):
            tail = pack(factor, listed((me + 1) % count, 0, room))
            left = lax.ppermute(tail, "cone", [(i, (i + 1) % count) for i in range(count)])
            head = pack(factor, listed((me + count - 1) % count, 2, room))
            right = lax.ppermute(head, "cone", [((i + 1) % count, i) for i in range(count)])
            near = own_grams(side, jnp.where(side == 1, place, 0), factor, move)
            left_at, right_at = jnp.where(side == 0, slots, 0), jnp.where(side == 2, slots, 0)
            return far_grams(side, left_at, right_at, left, right, move, near)

        return run

    rooms = [max(1, cones * eighth // 24) for eighth in (8, 10, 12)] + [cones]
    branch = (busiest > jnp.array(rooms[:-1], jnp.int32)).astype(jnp.int32).sum()
    gram_one = lax.switch(branch, [with_room(room) for room in rooms], leaf_factor, leaf_transfer)

    columns = eliminate(gram_one.reshape((parents * cones, rank, rank)), False)
    pairs = pack_pair(columns)
    segment = lax.all_gather(pairs, "cone", axis=0, tiled=False)
    every_factor = lax.all_gather(pairs, "box", axis=0, tiled=False)
    upper_one = jnp.transpose(columns, (2, 0, 1)).reshape((parents, cones, rank, rank))

    second, own_gram = second_level(parent_cone_map, segment, parent_transfer)
    group_size = LEAVES // parents
    summed = own_gram
    for bit_index in range(group_size.bit_length() - 1):
        summed = summed + partner_2(summed, "box", bit_index)
    inverse_two = jnp.transpose(eliminate(unfold(summed) / LEAVES, True), (2, 0, 1))
    new_transfer = jnp.einsum("bcij,ckj->bcik", second, inverse_two, precision=HIGH)
    projected = project(partner, live, upper_one, every_factor, coupling)
    return (projected, new_transfer)


def solution(mesh):
    in_specs = (
        P("box", "cone", None, None),
        P("box", "cone", None, None),
        P("cone"),
        P("box", "cone", None, None),
        P("cone"),
        P("box", "cone", None, None, None),
        P("box", "cone", None),
        P("box", "cone", None),
    )
    out_specs = (P("box", "cone", None, None, None), P("box", "cone", None, None))
    return jax.shard_map(shards, mesh=mesh, in_specs=in_specs, out_specs=out_specs, check_vma=False)
```
